32 devices in a mesh: fsdp: 8 (over z, y), tensor: 4 (over x, core).
Axes of the slice: x: 2, y: 2, z: 4, core: 2. Of those that a mesh axis runs over, the one named last changes fastest.
Arguments:
- activations: bfloat16 [8192, 5120], P('fsdp', 'tensor'), may hold values from -6 to 6
- cotangent: bfloat16 [8192, 5120], P('fsdp', 'tensor'), may hold values from -0.06591797 to 0.06591797
- weights: float32 [5120, 5120], P(None, ('tensor', 'fsdp')), may hold values from -0.025 to 0.025
- first_moment: float32 [5120, 5120], P(None, ('tensor', 'fsdp')), may hold values from -3 to 3
- second_moment: float32 [5120, 5120], P(None, ('tensor', 'fsdp')), may hold values from 0.01 to 1
Outputs:
- weights_new: float32 [5120, 5120], P('fsdp', 'tensor')
- first_new: float32 [5120, 5120], P('fsdp', 'tensor')
- second_new: float32 [5120, 5120], P('fsdp', 'tensor')
- weights_bf16: bfloat16 [5120, 5120], P(None, 'tensor')
The draws below stay inside these ranges and needn't reach their ends.
All inputs are finite; a program needn't handle non-finite values.
Results may differ from the reference program's by a relative error of at most 0.014.
Values may be sent and summed in bfloat16 or wider, within the bound.
A program may use at most 128 MiB of HBM per device.

```python
import math
import jax
import jax.numpy as jnp
from jax import lax

D = 5120
TOK_DEV = 1024
STEP = 20
TOKENS = 8192
N_FSDP = 8


def with_spikes(array, key, source, target, parts, factor):
    owner, partner = [(jnp.arange(array.shape[dim]) // (array.shape[dim] // parts)).reshape([-1 if axis == dim else 1 for axis in range(array.ndim)]) for dim in (source, target)]
    chosen = jax.random.permutation(key, parts)[partner]
    strong = (owner == chosen) | (owner == (partner + parts // 2) % parts)
    return jnp.where(strong, factor * array, array)


def block_levels(key, extent, split, low, largest):
    factor_of = 1.0
    for dim, blocks in split:
        heights = jax.random.uniform(jax.random.fold_in(jax.random.fold_in(key, 6), dim), (blocks,), jnp.float32, low / len(split), largest / len(split))
        factor_of = factor_of * jnp.repeat(jnp.exp(heights), extent[dim] // blocks).reshape((-1,) + (1,) * (len(extent) - 1 - dim))
    return factor_of


def normal_values(stream_key, extent, scale, most, pieces=(), kind=jnp.bfloat16):
    array = scale * jax.random.normal(stream_key, extent, jnp.float32)
    if pieces:
        array = array * block_levels(stream_key, extent, pieces, -0.22, 0.18)
    return jnp.clip(array, -most, most).astype(kind)


def heavy_noise(own_key, dims, deviation, reach, split, heavy, dtype=jnp.bfloat16):
    values = deviation * jax.random.normal(own_key, dims, jnp.float32)
    if split:
        values = values * block_levels(own_key, dims, split, -0.22, 0.18)
    return jnp.clip(with_spikes(values, jax.random.fold_in(own_key, 3), *heavy), -reach, reach).astype(dtype)


def setup_inputs(seed: int = 0) -> dict:
    arg_keys = jax.random.split(jax.random.key(seed), 6)
    activations = heavy_noise(arg_keys[0], (TOKENS, D), 1.0, 6.0, ((0, 8), (1, 4)), (0, 1, 8, 2.0))
    cotangent = normal_values(arg_keys[1], (TOKENS, D), (1.0 / TOKENS ** 0.5), 0.06591797, ((0, 8), (1, 4)))
    weights = normal_values(arg_keys[2], (D, D), 0.004, 0.025, ((1, 32),), jnp.float32)
    first_moment = normal_values(arg_keys[3], (D, D), 0.5, 3.0, ((1, 32),), jnp.float32)
    second_moment = jnp.clip(jnp.exp(math.log(1.0) - 4.6051702 * jax.random.uniform(arg_keys[4], (D, D), jnp.float32) ** block_levels(arg_keys[4], (D, D), ((1, 32),), -0.2, 0.2)), 0.01, 1.0)
    return {"activations": activations, "cotangent": cotangent, "weights": weights, "first_moment": first_moment, "second_moment": second_moment}


beta_one = 0.9
beta_two = 0.95
adam_eps = 1e-08
learn_rate = 0.0003
decay_rate = 0.1

def adam_update(weights, first_moment, second_moment, gradient):
    first_new = beta_one * first_moment + (1.0 - beta_one) * gradient
    second_new = beta_two * second_moment + (1.0 - beta_two) * gradient * gradient
    corrected = first_new / (1.0 - beta_one ** STEP)
    scaled = jnp.sqrt(second_new / (1.0 - beta_two ** STEP)) + adam_eps
    weights_new = weights - learn_rate * (corrected / scaled + decay_rate * weights)
    return (weights_new, first_new, second_new)

def reference(activations, cotangent, weights, first_moment, second_moment):
    token_blocks = activations.reshape(N_FSDP, TOK_DEV, D)
    cotangent_blocks = cotangent.reshape(N_FSDP, TOK_DEV, D)

    def accumulate(running, block_pair):
        product = lax.dot_general(block_pair[0].astype(jnp.float32), block_pair[1].astype(jnp.float32), (((0,), (0,)), ((), ())))
        rounded = lax.optimization_barrier(product.astype(jnp.bfloat16))
        return (running + rounded.astype(jnp.float32), None)
    gradient, unused = lax.scan(accumulate, jnp.zeros((D, D), jnp.float32), (token_blocks, cotangent_blocks))
    weights_new, first_new, second_new = adam_update(weights, first_moment, second_moment, gradient)
    return (weights_new, first_new, second_new, weights_new.astype(jnp.bfloat16))
```

```python
import functools

import jax
import jax.numpy as jnp
from jax import lax
from jax.experimental import pallas as pl
from jax.experimental.pallas import tpu as pltpu
from jax.sharding import PartitionSpec as P


STEP = 20


beta_one = 0.9
beta_two = 0.95
adam_eps = 1e-08
learn_rate = 0.0003
decay_rate = 0.1


def adam_update(weights, first_moment, second_moment, gradient):
    first_new = beta_one * first_moment + (1.0 - beta_one) * gradient
    second_new = beta_two * second_moment + (1.0 - beta_two) * gradient * gradient
    corrected = first_new / (1.0 - beta_one**STEP)
    scaled = jnp.sqrt(second_new / (1.0 - beta_two**STEP)) + adam_eps
    weights_new = weights - learn_rate * (corrected / scaled + decay_rate * weights)
    return (weights_new, first_new, second_new)


def line_pairs(length, step, senders):
    return [
        (2 * z + p, 2 * (z + step) + p)
        for z in range(length)
        for p in range(2)
        if senders(z) and 0 <= z + step < length
    ]


def reduce_line(term, z, length):
    last = length - 1
    right = left = None
    for s in range(last):
        up = term(jnp.clip(last + z - s, 0, last))
        down = term(jnp.clip(s - last + z, 0, last))
        if s:
            up = (up.astype(jnp.float32) + right.astype(jnp.float32)).astype(jnp.bfloat16)
            down = (down.astype(jnp.float32) + left.astype(jnp.float32)).astype(jnp.bfloat16)
        right = lax.ppermute(up, "fsdp", line_pairs(length, 1, lambda i: i <= s))
        left = lax.ppermute(down, "fsdp", line_pairs(length, -1, lambda i: i >= last - s))
    own = term(z)
    own = own.astype(jnp.float32)
    if last:
        own = own + right.astype(jnp.float32) + left.astype(jnp.float32)
    return own


def gather_kernel(
    length, own_ref, out_ref, local_sem, y_send, y_recv, r_send, r_recv, l_send, l_recv
):
    f = lax.axis_index("fsdp")
    z, p = f // 2, f % 2
    last = length - 1
    rows = own_ref.shape[0]
    pair, right, left = f + 1 - 2 * p, f + 2, f - 2

    def block(c):
        return out_ref.at[pl.ds((2 * c + p) * rows, rows)]

    def copy(src, dst, send, recv, target):
        return pltpu.make_async_remote_copy(
            src_ref=src,
            dst_ref=dst,
            send_sem=send,
            recv_sem=recv,
            device_id={"fsdp": target},
            device_id_type=pl.DeviceIdType.MESH,
        )

    def to_pair(c, src=None):
        return copy(block(c) if src is None else src, block(c), y_send.at[c], y_recv.at[c], pair)

    def to_right(s, src=None):
        c = z - s
        return copy(block(c) if src is None else src, block(c), r_send.at[s], r_recv.at[s], right)

    def to_left(s, src=None):
        c = z + s
        return copy(block(c) if src is None else src, block(c), l_send.at[s], l_recv.at[s], left)

    barrier = pltpu.get_barrier_semaphore()
    pl.semaphore_signal(
        barrier, inc=1, device_id={"fsdp": pair}, device_id_type=pl.DeviceIdType.MESH
    )

    @pl.when(z > 0)
    def _():
        pl.semaphore_signal(
            barrier, inc=1, device_id={"fsdp": left}, device_id_type=pl.DeviceIdType.MESH
        )

    @pl.when(z < last)
    def _():
        pl.semaphore_signal(
            barrier, inc=1, device_id={"fsdp": right}, device_id_type=pl.DeviceIdType.MESH
        )

    span = max(last, 1)
    pl.semaphore_wait(barrier, 1 + (z + span - 1) // span + (last - z + span - 1) // span)

    @pl.when(z < last)
    def _():
        to_right(0, own_ref).start()

    @pl.when(z > 0)
    def _():
        to_left(0, own_ref).start()

    to_pair(z, own_ref).start()
    here = pltpu.make_async_copy(own_ref, block(z), local_sem)
    here.start()

    for s in range(last):

        @pl.when(z > s)
        def _():
            c = z - 1 - s
            copy(block(c), block(c), r_send.at[s], r_recv.at[s], left).wait_recv()
            if s + 1 < last:

                @pl.when(z < last)
                def _():
                    to_right(s + 1).start()

            to_pair(c).start()

        @pl.when(z < last - s)
        def _():
            c = z + 1 + s
            copy(block(c), block(c), l_send.at[s], l_recv.at[s], right).wait_recv()
            if s + 1 < last:

                @pl.when(z > 0)
                def _():
                    to_left(s + 1).start()

            to_pair(c).start()

    for s in range(last):

        @pl.when((z < last) & (z >= s))
        def _():
            to_right(s).wait_send()

        @pl.when((z > 0) & (last - z >= s))
        def _():
            to_left(s).wait_send()

    here.wait()
    for c in range(length):
        to_pair(c).wait_send()
        theirs = out_ref.at[pl.ds((2 * c + 1 - p) * rows, rows)]
        copy(theirs, theirs, y_send.at[c], y_recv.at[c], pair).wait_recv()


def gather_line(own, length):
    rows, cols = own.shape
    dma = pltpu.SemaphoreType.DMA
    steps = max(length - 1, 1)
    return pl.pallas_call(
        functools.partial(gather_kernel, length),
        out_shape=jax.ShapeDtypeStruct((2 * length * rows, cols), own.dtype),
        in_specs=[pl.BlockSpec(memory_space=pltpu.VMEM)],
        out_specs=pl.BlockSpec(memory_space=pl.ANY),
        scratch_shapes=[dma, dma((length,)), dma((length,))] + [dma((steps,))] * 4,
        compiler_params=pltpu.CompilerParams(collective_id=0, has_side_effects=True),
        name="gather_rows",
    )(own)


def body(activations, cotangent, weights, first_moment, second_moment, *, n, parts):
    f = lax.axis_index("fsdp")
    z, p = f // 2, f % 2
    length = n // 2
    depth, cols = weights.shape
    rows = depth // n
    tok, width = activations.shape
    pair = [(i, i ^ 1) for i in range(n)]

    packed = jnp.concatenate([weights, first_moment, second_moment], axis=1).astype(jnp.bfloat16)
    lines = [[2 * i + q for i in range(length)] for q in range(2)]
    packed = lax.optimization_barrier(packed.reshape(length, 2, rows, 3 * cols))
    along = lax.all_to_all(packed, "fsdp", 0, 0, axis_index_groups=lines)
    blocks = activations.reshape(tok, width // (2 * rows), 2, rows)
    keep = lax.dynamic_index_in_dim(blocks, p, 2, False).reshape(tok, width // 2)
    give = lax.dynamic_index_in_dim(blocks, 1 - p, 2, False).reshape(tok, width // 2)
    got = lax.ppermute(give, "fsdp", pair)
    cot_peer = lax.ppermute(cotangent, "fsdp", pair)
    mine = lax.all_gather(keep, "tensor")
    theirs = lax.all_gather(got, "tensor")

    def product(a, b):
        return lax.dot_general(a, b, (((0,), (0,)), ((), ())), preferred_element_type=jnp.float32)

    groups = length // parts

    def term(c):
        at = (c // groups, 0, (c % groups) * rows)
        near, far = (
            lax.dynamic_slice(array, at, (1, tok, rows))[0] for array in (mine, theirs)
        )
        total = product(near, cotangent) + product(far, cot_peer)
        return lax.optimization_barrier(total.astype(jnp.bfloat16))

    gradient = reduce_line(term, z, length)

    stay = lax.dynamic_index_in_dim(along, p, 1, False)
    across = lax.ppermute(lax.dynamic_index_in_dim(along, 1 - p, 1, False), "fsdp", pair)
    moved = jnp.where(p == 0, jnp.stack([stay, across], 1), jnp.stack([across, stay], 1))

    def owned(k):
        pieces = [moved[i // 2, i % 2, :, k * cols : (k + 1) * cols] for i in range(n)]
        return lax.optimization_barrier(jnp.concatenate(pieces, axis=1)).astype(jnp.float32)

    weights_new, first_new, second_new = adam_update(owned(0), owned(1), owned(2), gradient)
    rounded = weights_new.astype(jnp.bfloat16)
    weights_bf16 = gather_line(rounded, length)
    return (weights_new, first_new, second_new, weights_bf16)


def solution(mesh):
    n, parts = mesh.shape["fsdp"], mesh.shape["tensor"]

    def run(*arrays):
        return body(*arrays, n=n, parts=parts)

    return jax.shard_map(
        run,
        mesh=mesh,
        in_specs=(
            P("fsdp", "tensor"),
            P("fsdp", "tensor"),
            P(None, ("tensor", "fsdp")),
            P(None, ("tensor", "fsdp")),
            P(None, ("tensor", "fsdp")),
        ),
        out_specs=(
            P("fsdp", "tensor"),
            P("fsdp", "tensor"),
            P("fsdp", "tensor"),
            P(None, "tensor"),
        ),
        check_vma=False,
    )
```
